32 devices in a mesh: grp: 2 (over y), row: 16 (over z, x, core).
Axes of the slice: x: 2, y: 2, z: 4, core: 2. Of those that a mesh axis runs over, the one named last changes fastest.
Arguments:
- item_ids: int32 [128, 512], P(('grp', 'row')), may hold values from 0 to 49999, as said below
- lengths: int32 [128], P(('grp', 'row')), may hold values from 358 to 512
- target_ids: int32 [128, 512], P(('grp', 'row')), may hold values from 0 to 49999
- target_logq: bfloat16 [128, 512], P(('grp', 'row')), may hold values from -4 to 0
- negative_ids: int32 [2048], P(('grp', 'row')), may hold values from 0 to 49999
- negative_logq: bfloat16 [2048], P(('grp', 'row')), may hold values from -4 to 0
- table_weight: float32 [50000, 256], P('row'), may hold values from -0.6 to 0.6
- table_accum: float32 [50000], P('row'), may hold values from 1.1737531e-13 to 4.6950123e-13
- dense_weight: float32 [256, 4608], P(None, ('grp', 'row')), may hold values from -0.375 to 0.375
- dense_first: float32 [256, 4608], P(None, ('grp', 'row')), may hold values from -2.861023e-06 to 2.861023e-06
- dense_second: float32 [256, 4608], P(None, ('grp', 'row')), may hold values from 3.390842e-15 to 1.3563368e-14
- gain_weight: float32 [3, 256], replicated, may hold values from 0.5 to 1.5
- gain_first: float32 [3, 256], replicated, may hold values from -3.0517578e-05 to 3.0517578e-05
- gain_second: float32 [3, 256], replicated, may hold values from 3.390842e-13 to 1.3563368e-12
Outputs:
- mean_loss: float32 [], replicated
- grad_norm: float32 [], replicated
- new_table: float32 [50000, 256], P('row')
- table_grad: float32 [50000, 256], P('row')
- new_accum: float32 [50000], P('row')
- table_copy: bfloat16 [50000, 256], P('row')
- new_dense: float32 [256, 4608], P(None, ('grp', 'row'))
- new_first: float32 [256, 4608], P(None, ('grp', 'row'))
- new_second: float32 [256, 4608], P(None, ('grp', 'row'))
- dense_copy: bfloat16 [256, 4608], P(None, ('grp', 'row'))
- new_gains: float32 [3, 256], replicated
- new_gain_first: float32 [3, 256], replicated
- new_gain_second: float32 [3, 256], replicated
The draws below stay inside these ranges and needn't reach their ends.
Inputs may be any that keep to these rules, and one draw needn't show every extreme that they name: `item_ids`: taking one device's item ids, target ids and negative ids together, at most 520 of them name rows with the same id // 3125; in each group some value of id // 3125 is named exactly 520 times by every device of the group.
All inputs are finite; a program needn't handle non-finite values.
Results may differ from the reference program's by a relative error of at most 0.0093.
The reference program's roundings to bfloat16 on the way count: a program that leaves them out, or rounds other values in their place, can miss the bound.
Values may be sent and summed in bfloat16 or wider, within the bound.
A program may use at most 256 MiB of HBM per device.

```python
import math
import jax
import jax.numpy as jnp
from jax import lax

D = 256
HEADS = 8
HDIM = 64
FF = 1024
L = 512
ROWS_DEV = 3125
SEQ_DEV = 4
STEP = 10
VOCAB = 50000
COLS = 4608
SEQS = 128
NEGS = 2048
NNEG = 1024
PEERS = 16
REQS = 4160
CAP = 520
N_GRP = 2
N_ROW = 16


def request_plan(key):
    key = jax.random.fold_in(key, 5)
    members = SEQS // SEQ_DEV
    groups = members // PEERS
    full_owner = jax.random.randint(jax.random.fold_in(key, 1), (groups,), 0, PEERS)
    tickets = jnp.repeat(jnp.arange(PEERS, dtype=jnp.int32), CAP)

    def member_ids(member):
        own_key = jax.random.fold_in(key, member + 2)
        key_order, key_shuffle, key_offset = jax.random.split(own_key, 3)
        order = jax.random.permutation(key_order, PEERS * CAP).astype(jnp.int32)
        ranking = jnp.where(tickets == full_owner[member // PEERS], 0, 1) * (PEERS * CAP) + order
        chosen = tickets[jnp.argsort(ranking)][:REQS]
        chosen = jax.random.permutation(key_shuffle, chosen)
        offsets = jax.random.randint(key_offset, (REQS,), 0, ROWS_DEV)
        return (chosen * ROWS_DEV + offsets).astype(jnp.int32)
    return jax.vmap(member_ids)(jnp.arange(members))


def draw_item_ids(key, part):
    return request_plan(key)[:, :SEQ_DEV * L].reshape(SEQS, L)


def draw_target_ids(key, part):
    return request_plan(key)[:, SEQ_DEV * L:2 * SEQ_DEV * L].reshape(SEQS, L)


def draw_negative_ids(key, part):
    return request_plan(key)[:, 2 * SEQ_DEV * L:].reshape(NEGS)


def touch_ends(result, rng, low, high):
    dims = result.shape
    place = [jax.random.randint(jax.random.fold_in(rng, axis), (), 0, dims[axis]) for axis in range(len(dims))]
    result = result.at[tuple(place)].set(low)
    longest = dims.index(max(dims))
    place[longest] = (place[longest] + 1) % dims[longest]
    return result.at[tuple(place)].set(high)


def steps_of(key, dims, cuts, smallest, largest):
    level = 1.0
    for dim, blocks in cuts:
        steps = jax.random.uniform(jax.random.fold_in(jax.random.fold_in(key, 6), dim), (blocks,), jnp.float32, smallest / len(cuts), largest / len(cuts))
        level = level * jnp.repeat(jnp.exp(steps), dims[dim] // blocks).reshape((-1,) + (1,) * (len(dims) - 1 - dim))
    return level


def bell_draw(key, dims, scale, reach, shards=(), held_as=jnp.bfloat16):
    loudness = steps_of(key, dims, shards, -0.22, 0.18) if shards else 1.0
    entries = jax.random.normal(key, dims, jnp.float32) * scale * loudness
    return jnp.minimum(jnp.maximum(entries, -reach), reach).astype(held_as)


def setup_inputs(seed: int = 0) -> dict:
    streams_of = jax.random.split(jax.random.key(seed), 15)
    item_ids = draw_item_ids(jax.random.fold_in(streams_of[14], 71), 0)
    lengths = touch_ends(jax.random.randint(streams_of[1], (SEQS,), 7 * L // 10, L + 1), jax.random.fold_in(streams_of[1], 1), 7 * L // 10, L).astype(jnp.int32)
    target_ids = draw_target_ids(jax.random.fold_in(streams_of[14], 71), 0)
    target_logq = jnp.clip(-4.0 + 4.0 * jax.random.uniform(streams_of[3], (SEQS, L), jnp.float32) ** steps_of(streams_of[3], (SEQS, L), ((0, 32),), -0.2, 0.2), -4.0, 0.0).astype(jnp.bfloat16)
    negative_ids = draw_negative_ids(jax.random.fold_in(streams_of[14], 71), 0)
    negative_logq = jnp.clip(-4.0 + 4.0 * jax.random.uniform(streams_of[5], (NEGS,), jnp.float32) ** steps_of(streams_of[5], (NEGS,), ((0, 32),), -0.2, 0.2), -4.0, 0.0).astype(jnp.bfloat16)
    table_weight = bell_draw(streams_of[6], (VOCAB, D), 0.1, 0.6, ((0, 16),), jnp.float32)
    table_accum = jnp.clip(jnp.exp(math.log(4.695012282597555e-13) - 1.3862944 * jax.random.uniform(streams_of[7], (VOCAB,), jnp.float32) ** steps_of(streams_of[7], (VOCAB,), ((0, 16),), -0.2, 0.2)), 1.1737530706493887e-13, 4.695012282597555e-13)
    dense_weight = bell_draw(streams_of[8], (D, COLS), D ** -0.5, 0.375, ((1, 32),), jnp.float32)
    dense_first = bell_draw(streams_of[9], (D, COLS), (0.111 * 0.002 / (D * COLS) ** 0.5), 2.86102294921875e-06, ((1, 32),), jnp.float32)
    dense_second = jnp.clip(jnp.exp(math.log(1.3563368330760713e-14) - 1.3862944 * jax.random.uniform(streams_of[10], (D, COLS), jnp.float32) ** steps_of(streams_of[10], (D, COLS), ((1, 32),), -0.2, 0.2)), 3.3908420826901783e-15, 1.3563368330760713e-14)
    gain_weight = jnp.clip(1.0 + 0.1 * jax.random.normal(streams_of[11], (3, D), jnp.float32), 0.5, 1.5)
    gain_first = bell_draw(streams_of[12], (3, D), (1.11 * 0.002 / (D * COLS) ** 0.5), 3.0517578125e-05, (), jnp.float32)
    gain_second = jnp.clip(jnp.exp(jax.random.uniform(streams_of[13], (3, D), jnp.float32, math.log(3.390842023397872e-13), math.log(1.3563368093591488e-12))), 3.390842023397872e-13, 1.3563368093591488e-12)
    return dict(item_ids=item_ids, lengths=lengths, target_ids=target_ids, target_logq=target_logq, negative_ids=negative_ids, negative_logq=negative_logq, table_weight=table_weight, table_accum=table_accum, dense_weight=dense_weight, dense_first=dense_first, dense_second=dense_second, gain_weight=gain_weight, gain_first=gain_first, gain_second=gain_second)


@jax.custom_vjp
def low(v):
    return lax.optimization_barrier(v.astype(jnp.bfloat16)).astype(jnp.float32)

@jax.custom_vjp
def low_back(v):
    return v

def low_keep(v):
    return (low(v), None)

def low_pass(kept, grad):
    return (grad,)

def back_keep(v):
    return (v, None)

def back_low(kept, grad):
    return (low(grad),)
low.defvjp(low_keep, low_pass)
low_back.defvjp(back_keep, back_low)
highest = lax.Precision.HIGHEST
clip_level = 0.002
adam_rate = 0.05
gains_rate = 0.6
rows_rate = 0.05
beta_one = 0.9
beta_two = 0.999
adam_eps = 1e-08
decay_rate = 0.01

def matmul(left, right):
    return jnp.dot(left, right, precision=highest)

def norm_apply(values, gain):
    return values * lax.rsqrt(lax.optimization_barrier(jnp.mean(values * values, -1, keepdims=True)) + 1e-06) * gain

def split_dense(weights):
    inner = HEADS * HDIM
    return (weights[:, :3 * inner], weights[:, 3 * inner:4 * inner], weights[:, 4 * inner:4 * inner + FF], weights[:, 4 * inner + FF:4 * inner + 2 * FF], weights[:, 4 * inner + 2 * FF:])

def sequence_loss(weights, gain_rows, hist_rows, target_rows, target_bias, is_valid, neg_rows, neg_bias):
    query_key_value_weight, output_weight, up_weight, down_weight, pos_table = split_dense(weights)
    inner = HEADS * HDIM
    embedded_tokens = hist_rows + pos_table.T
    normed = low(norm_apply(embedded_tokens, gain_rows[0]))
    mixed_state = low(low_back(matmul(normed, query_key_value_weight)))
    queries = mixed_state[:, :inner].reshape(L, HEADS, HDIM)
    keys_all = mixed_state[:, inner:2 * inner].reshape(L, HEADS, HDIM)
    values_all = mixed_state[:, 2 * inner:].reshape(L, HEADS, HDIM)
    scores = low_back(jnp.einsum('qhd,khd->hqk', queries, keys_all, precision=highest) * 0.125)
    causal = lax.broadcasted_iota(jnp.int32, (L, L), 0) >= lax.broadcasted_iota(jnp.int32, (L, L), 1)
    scores = jnp.where(causal[None], scores, -1e+30)
    attn_probs = low(jax.nn.softmax(scores, -1))
    attention_context = jnp.einsum('hqk,khd->qhd', attn_probs, values_all, precision=highest).reshape(L, inner)
    attention_context = low(low_back(attention_context))
    after_attention_state = embedded_tokens + low_back(jnp.dot(attention_context, output_weight.T, precision=highest))
    normed_two = low(norm_apply(after_attention_state, gain_rows[1]))
    hidden_preactivation = low_back(matmul(normed_two, up_weight))
    hidden = low(jax.nn.gelu(hidden_preactivation, approximate=True))
    after_ffn = after_attention_state + low_back(jnp.dot(hidden, down_weight.T, precision=highest))
    states = low(norm_apply(after_ffn, gain_rows[2]))
    pos_logit = lax.optimization_barrier(jnp.sum(states * target_rows, -1)) - target_bias
    neg_logit = low_back(jnp.dot(states, neg_rows.T, precision=highest)) - neg_bias[None, :]
    log_total = jax.nn.logsumexp(jnp.concatenate([pos_logit[:, None], neg_logit], 1), 1)
    return jnp.sum(jnp.where(is_valid, log_total - pos_logit, 0.0))

def adam_update(weight, first, second, grad, decay, rate):
    first_new = beta_one * first + (1.0 - beta_one) * grad
    second_new = beta_two * second + (1.0 - beta_two) * grad * grad
    fix_one = 1.0 - beta_one ** STEP
    fix_two = 1.0 - beta_two ** STEP
    weight_new = weight - rate * (first_new / fix_one / (jnp.sqrt(second_new / fix_two) + adam_eps) + decay * weight)
    return (weight_new, first_new, second_new)

def reference(item_ids, lengths, target_ids, target_logq, negative_ids, negative_logq, table_weight, table_accum, dense_weight, dense_first, dense_second, gain_weight, gain_first, gain_second):
    is_valid = lax.broadcasted_iota(jnp.int32, (SEQS, L), 1) < lengths[:, None]
    event_count = jnp.sum(is_valid.astype(jnp.float32))
    inverse = 1.0 / event_count
    groups = (jnp.arange(SEQS) // (SEQ_DEV * N_ROW)).astype(jnp.int32)
    target_bias = target_logq.astype(jnp.float32)
    neg_bias = negative_logq.astype(jnp.float32).reshape(N_GRP, NNEG)

    def forward(dense, gain_rows, table):
        dense_low = low(dense)
        table_low = low(table)
        hist = table_low[item_ids]
        targets = table_low[target_ids]
        negs = table_low[negative_ids].reshape(N_GRP, NNEG, D)

        def one_sequence(total_sum, inputs):
            hist_one, target_one, bias_one, valid_one, group_one = inputs
            part_sum = jax.checkpoint(sequence_loss)(dense_low, gain_rows, hist_one, target_one, bias_one, valid_one, negs[group_one], neg_bias[group_one])
            return (total_sum + part_sum, None)
        total_sum, _ = lax.scan(one_sequence, jnp.zeros((), jnp.float32), (hist, targets, target_bias, is_valid, groups))
        return total_sum * inverse
    mean_loss, pull = jax.vjp(forward, dense_weight, gain_weight, table_weight)
    grad_dense, grad_gain, grad_table = pull(jnp.ones((), mean_loss.dtype))
    grad_norm = jnp.sqrt(jnp.sum(grad_dense * grad_dense) + jnp.sum(grad_gain * grad_gain) + jnp.sum(grad_table * grad_table))
    factor = jnp.minimum(1.0, clip_level / grad_norm)
    table_grad = grad_table * factor
    new_accum = table_accum + lax.optimization_barrier(jnp.mean(table_grad * table_grad, -1))
    new_table = table_weight - rows_rate * table_grad / (jnp.sqrt(new_accum)[:, None] + adam_eps)
    new_dense, new_first, new_second = adam_update(dense_weight, dense_first, dense_second, grad_dense * factor, decay_rate, adam_rate)
    new_gains, new_gain_first, new_gain_second = adam_update(gain_weight, gain_first, gain_second, grad_gain * factor, 0.0, gains_rate)
    return (mean_loss, grad_norm, new_table, table_grad, new_accum, new_table.astype(jnp.bfloat16), new_dense, new_first, new_second, new_dense.astype(jnp.bfloat16), new_gains, new_gain_first, new_gain_second)
```

```python
import functools

import jax
import jax.numpy as jnp
from jax import lax
from jax.experimental import pallas as pl
from jax.experimental.pallas import tpu as pltpu
from jax.sharding import PartitionSpec as P

HEADS = 8
HDIM = 64
FF = 1024
STEP = 10
f32 = jnp.float32
bf16 = jnp.bfloat16

def mm(a, b):
    return lax.dot_general(a, b, (((1,), (0,)), ((), ())), preferred_element_type=f32)


def mm_t(a, b):
    return lax.dot_general(a, b, (((1,), (1,)), ((), ())), preferred_element_type=f32)


def t_mm(a, b):
    return lax.dot_general(a, b, (((0,), (0,)), ((), ())), preferred_element_type=f32)


GELU_C = 0.7978845608028654


def seq_kernel(
    len_ref, inv_ref,
    hist_ref, tgt_ref, tlq_ref, neg_ref, nlq_ref, wt_ref, gain_ref,
    demb_ref, dtgt_ref, gt_ref, ng_ref, gg_ref, loss_ref,
    emb, xn1, qkv, qh, kh, vh, dch, probs, ctx, aat, xn2, hid, gp, ffn, st, dneg, dst, dhid, dmx, gacc, nacc, rb,
):
    s = pl.program_id(0)
    last = pl.num_programs(0) - 1
    L, D = emb.shape
    inner = HEADS * HDIM
    O1 = 3 * inner
    O2 = O1 + inner
    O3 = O2 + FF
    O4 = O3 + FF
    RB = 128
    NB = L // RB

    @pl.when(s == 0)
    def _():
        @pl.loop(0, D // 16)
        def _(i):
            r = pl.ds(pl.multiple_of(i * 16, 16), 16)
            gacc[r, :] = jnp.zeros((16, gacc.shape[1]), f32)
            nacc[r, :] = jnp.zeros((16, nacc.shape[1]), f32)
        gt_ref[O4:, :] = jnp.zeros((L, D), f32)
        gg_ref[...] = jnp.zeros(gg_ref.shape, f32)
        loss_ref[...] = jnp.zeros(loss_ref.shape, f32)

    g1 = gain_ref[0:1, :]
    g2 = gain_ref[1:2, :]
    g3 = gain_ref[2:3, :]

    def rows(i):
        return pl.ds(pl.multiple_of(i * RB, RB), RB)

    def inv_rms(x):
        return lax.rsqrt(jnp.mean(x * x, -1, keepdims=True) + 1e-06)

    @pl.loop(0, NB)
    def _(i):
        r = rows(i)
        x = hist_ref[0, r, :].astype(f32) + wt_ref[pl.ds(pl.multiple_of(O4 + i * RB, RB), RB), :].astype(f32)
        emb[r, :] = x
        xn1[r, :] = (x * inv_rms(x) * g1).astype(bf16)

    qkv[...] = mm_t(xn1[...], wt_ref[0:O1, :]).astype(bf16)

    lane = lax.broadcasted_iota(jnp.int32, (1, 2 * HDIM), 1)

    def own(h):
        return (lane // HDIM) == (h % 2)

    @pl.loop(0, HEADS)
    def _(h):
        m = own(h)
        off = pl.multiple_of((h // 2) * 2 * HDIM, 2 * HDIM)
        zero = jnp.zeros((), bf16)
        qh[h] = jnp.where(m, qkv[:, pl.ds(off, 2 * HDIM)] * jnp.asarray(0.125, bf16), zero)
        kh[h] = jnp.where(m, qkv[:, pl.ds(pl.multiple_of(inner + off, 2 * HDIM), 2 * HDIM)], zero)
        vh[h] = jnp.where(m, qkv[:, pl.ds(pl.multiple_of(2 * inner + off, 2 * HDIM), 2 * HDIM)], zero)

    QB = 256
    NQ = L // QB
    causal = lax.broadcasted_iota(jnp.int32, (QB, QB), 0) >= lax.broadcasted_iota(jnp.int32, (QB, QB), 1)

    @pl.loop(0, HEADS // 2)
    def _(hp):
        off = pl.multiple_of(hp * 2 * HDIM, 2 * HDIM)
        for i in range(NQ):
            n = (i + 1) * QB
            q0 = i * QB
            acc = None
            for j in range(2):
                h = hp * 2 + j
                sc = mm_t(qh[h, q0:q0 + QB, :], kh[h, 0:n, :])
                tail = jnp.where(causal, sc[:, q0:], -1e30)
                sc = tail if i == 0 else jnp.concatenate([sc[:, :q0], tail], 1)
                e = jnp.exp(sc - jnp.max(sc, -1, keepdims=True))
                p = e / jnp.sum(e, -1, keepdims=True)
                probs[h, q0:q0 + QB, 0:n] = p
                c = mm(p.astype(bf16), vh[h, 0:n, :])
                acc = c if acc is None else acc + c
            ctx[q0:q0 + QB, pl.ds(off, 2 * HDIM)] = acc.astype(bf16)

    aat[...] = emb[...] + mm(ctx[...], wt_ref[O1:O2, :])

    @pl.loop(0, NB)
    def _(i):
        r = rows(i)
        x = aat[r, :]
        xn2[r, :] = (x * inv_rms(x) * g2).astype(bf16)

    gp[...] = mm_t(xn2[...], wt_ref[O2:O3, :])

    @pl.loop(0, L // 32)
    def _(i):
        r = pl.ds(pl.multiple_of(i * 32, 32), 32)
        x = gp[r, :]
        x2 = x * x
        t = jnp.tanh(GELU_C * (x + 0.044715 * (x2 * x)))
        half = 0.5 * (1.0 + t)
        hid[r, :] = (x * half).astype(bf16)
        gp[r, :] = half + (0.5 * GELU_C) * x * (1.0 - t * t) * (1.0 + (3 * 0.044715) * x2)

    ffn[...] = aat[...] + mm(hid[...], wt_ref[O3:O4, :])

    @pl.loop(0, NB)
    def _(i):
        r = rows(i)
        x = ffn[r, :]
        st[r, :] = (x * inv_rms(x) * g3).astype(bf16)

    inv = inv_ref[0, 0]
    length = len_ref[s]
    LB = 128
    eye = lax.broadcasted_iota(jnp.int32, (LB, LB), 0) == lax.broadcasted_iota(jnp.int32, (LB, LB), 1)

    @pl.loop(0, L // LB)
    def _(i):
        r = pl.ds(pl.multiple_of(i * LB, LB), LB)
        sl = st[r, :]
        sf = sl.astype(f32)
        tf = tgt_ref[0, r, :].astype(f32)
        tlq = jnp.sum(jnp.where(eye, tlq_ref[0, :, r], 0.0), 1, keepdims=True)
        pos = jnp.sum(sf * tf, -1, keepdims=True) - tlq
        neg = mm_t(sl, neg_ref[...]) - nlq_ref[...]
        top = jnp.maximum(jnp.max(neg, -1, keepdims=True), pos)
        e = jnp.exp(neg - top)
        total = jnp.exp(pos - top) + jnp.sum(e, -1, keepdims=True)
        lt = top + jnp.log(total)
        t_at = i * LB + lax.broadcasted_iota(jnp.int32, (LB, 1), 0)
        valid = (t_at < length).astype(f32)
        loss_ref[...] += jnp.sum(valid * (lt - pos))
        d_pos = valid * inv * (jnp.exp(pos - lt) - 1.0)
        dn = (e * (valid * inv / total)).astype(bf16)
        dneg[r, :] = dn
        dtgt_ref[0, r, :] = (d_pos * sf).astype(bf16)
        dst[r, :] = d_pos * tf + mm(dn, neg_ref[...])

    nacc[...] += t_mm(st[...], dneg[...])

    def norm_back(x, dy, g):
        r = inv_rms(x)
        xh = x * r
        dg = jnp.sum(dy * xh, 0, keepdims=True)
        dyg = dy * g
        dx = r * (dyg - xh * jnp.mean(dyg * xh, -1, keepdims=True))
        return dx, dg

    @pl.loop(0, NB)
    def _(i):
        r = rows(i)
        dx, dg = norm_back(ffn[r, :], dst[r, :], g3)
        gg_ref[2:3, :] += dg
        dst[r, :] = dx
        rb[r, :] = dx.astype(bf16)

    gacc[:, O3:O4] += t_mm(rb[...], hid[...])
    gp[...] = mm_t(rb[...], wt_ref[O3:O4, :]) * gp[...]
    dhid[...] = gp[...].astype(bf16)
    gacc[:, O2:O3] += t_mm(xn2[...], dhid[...])
    ffn[...] = mm(dhid[...], wt_ref[O2:O3, :])

    @pl.loop(0, NB)
    def _(i):
        r = rows(i)
        dx, dg = norm_back(aat[r, :], ffn[r, :], g2)
        gg_ref[1:2, :] += dg
        d = dst[r, :] + dx
        dst[r, :] = d
        rb[r, :] = d.astype(bf16)

    gacc[:, O1:O2] += t_mm(rb[...], ctx[...])
    ctx[...] = mm_t(rb[...], wt_ref[O1:O2, :]).astype(bf16)

    @pl.loop(0, HEADS)
    def _(h):
        off = pl.multiple_of((h // 2) * 2 * HDIM, 2 * HDIM)
        dch[h] = jnp.where(own(h), ctx[:, pl.ds(off, 2 * HDIM)], jnp.zeros((), bf16))

    @pl.loop(0, HEADS // 2)
    def _(hp):
        off = pl.multiple_of(hp * 2 * HDIM, 2 * HDIM)
        dk = [None] * NQ
        dv = [None] * NQ
        for i in range(NQ):
            n = (i + 1) * QB
            q0 = i * QB
            dq = None
            for j in range(2):
                h = hp * 2 + j
                p = probs[h, q0:q0 + QB, 0:n]
                dc = dch[h, q0:q0 + QB, :]
                dp = mm_t(dc, vh[h, 0:n, :])
                ds = (p * (dp - jnp.sum(p * dp, -1, keepdims=True))).astype(bf16)
                pb = p.astype(bf16)
                c = mm(ds, kh[h, 0:n, :])
                dq = c if dq is None else dq + c
                qb = qh[h, q0:q0 + QB, :]
                for b in range(i + 1):
                    k0 = b * QB
                    a = t_mm(ds[:, k0:k0 + QB], qb)
                    dk[b] = a if dk[b] is None else dk[b] + a
                    a = t_mm(pb[:, k0:k0 + QB], dc)
                    dv[b] = a if dv[b] is None else dv[b] + a
            dmx[q0:q0 + QB, pl.ds(off, 2 * HDIM)] = (dq * 0.125).astype(bf16)
        for b in range(NQ):
            k0 = b * QB
            dmx[k0:k0 + QB, pl.ds(pl.multiple_of(inner + off, 2 * HDIM), 2 * HDIM)] = dk[b].astype(bf16)
            dmx[k0:k0 + QB, pl.ds(pl.multiple_of(2 * inner + off, 2 * HDIM), 2 * HDIM)] = dv[b].astype(bf16)

    gacc[:, 0:O1] += t_mm(xn1[...], dmx[...])
    ffn[...] = mm(dmx[...], wt_ref[0:O1, :])

    @pl.loop(0, NB)
    def _(i):
        r = rows(i)
        dx, dg = norm_back(emb[r, :], ffn[r, :], g1)
        gg_ref[0:1, :] += dg
        d = dst[r, :] + dx
        demb_ref[0, r, :] = d.astype(bf16)
        gt_ref[pl.ds(pl.multiple_of(O4 + i * RB, RB), RB), :] += d

    @pl.when(s == last)
    def _():
        @pl.loop(0, O4 // 128)
        def _(i):
            c = pl.ds(pl.multiple_of(i * 128, 128), 128)
            gt_ref[c, :] = gacc[:, c].T

        @pl.loop(0, nacc.shape[1] // 128)
        def _(i):
            c = pl.ds(pl.multiple_of(i * 128, 128), 128)
            ng_ref[c, :] = nacc[:, c].T.astype(bf16)


def seq_step(lengths, inverse, hist, tgt, tlq, neg, nlq, wt, gains, interpret=False):
    S, L, D = hist.shape
    N = neg.shape[0]
    C = wt.shape[0]
    inner = HEADS * HDIM
    whole = lambda *shape: pl.BlockSpec(shape, lambda s: (0,) * len(shape))
    once = lambda *shape: pl.BlockSpec(shape, lambda s: (0,) * len(shape), pipeline_mode=pl.Buffered(1))
    per = pl.BlockSpec((1, L, D), lambda s: (s, 0, 0))
    V = pltpu.VMEM
    return pl.pallas_call(
        seq_kernel,
        grid=(S,),
        in_specs=[
            pl.BlockSpec(memory_space=pltpu.SMEM),
            pl.BlockSpec(memory_space=pltpu.SMEM),
            per, per,
            pl.BlockSpec((1, 1, L), lambda s: (s, 0, 0)),
            once(N, D), once(1, N), once(C, D), once(*gains.shape),
        ],
        out_specs=[per, per, whole(C, D), whole(N, D), whole(8, D), whole(1, 1)],
        out_shape=[
            jax.ShapeDtypeStruct((S, L, D), bf16),
            jax.ShapeDtypeStruct((S, L, D), bf16),
            jax.ShapeDtypeStruct((C, D), f32),
            jax.ShapeDtypeStruct((N, D), bf16),
            jax.ShapeDtypeStruct((8, D), f32),
            jax.ShapeDtypeStruct((1, 1), f32),
        ],
        scratch_shapes=[
            V((L, D), f32), V((L, D), bf16), V((L, 3 * inner), bf16),
            V((HEADS, L, 128), bf16), V((HEADS, L, 128), bf16), V((HEADS, L, 128), bf16), V((HEADS, L, 128), bf16),
            V((HEADS, L, L), f32), V((L, inner), bf16), V((L, D), f32), V((L, D), bf16),
            V((L, FF), bf16), V((L, FF), f32), V((L, D), f32), V((L, D), bf16),
            V((L, N), bf16), V((L, D), f32), V((L, FF), bf16), V((L, 3 * inner), bf16),
            V((D, C - L), f32), V((D, N), f32), V((L, D), bf16),
        ],
        compiler_params=pltpu.CompilerParams(vmem_limit_bytes=60 * 1024 * 1024, dimension_semantics=("arbitrary",)),
        name="seq_step",
        interpret=interpret,
    )(lengths, inverse, hist, tgt, tlq, neg, nlq, wt, gains)


MESH = pl.DeviceIdType.MESH


def gather_kernel(Z, X, parts, tab, wts, meta, table, wfull, mfull, send, recv, local):
    g = lax.axis_index("grp")
    row = lax.axis_index("row")
    z = row // (2 * X)
    x = (row // 2) % X
    c = row % 2
    K = len(parts) + 4
    KW = len(parts)
    KM = KW + 2

    def at(z_, x_, c_):
        return z_ * (2 * X) + x_ * 2 + c_

    nbr = {
        "up": (g, at(z + 1, x, c)), "dn": (g, at(z - 1, x, c)),
        "x": (g, at(z, 1 - x, c)), "y": (1 - g, row), "c": (g, at(z, x, 1 - c)),
    }
    has = {"up": z + 1 < Z, "dn": z > 0, "x": None, "y": None, "c": None}
    dirs = ("up", "dn", "x", "y", "c")

    def when(cond, f):
        if cond is None:
            f()
        else:
            pl.when(cond)(f)

    bar = pltpu.get_barrier_semaphore()
    for d in dirs:
        when(has[d], lambda d=d: pl.semaphore_signal(bar, inc=1, device_id=nbr[d], device_id_type=MESH))
    pl.semaphore_wait(bar, 3 + (z + 1 < Z).astype(jnp.int32) + (z > 0).astype(jnp.int32))

    def place(k, s, gg):
        if k < KW:
            st, size, _ = parts[k]
            return table.at[s, pl.ds(st, size), :]
        if k < KM:
            return wfull.at[gg * (2 * X * Z) + s]
        return mfull.at[gg * (2 * X * Z) + s]

    def origin(k):
        if k < KW:
            st, size, _ = parts[k]
            return tab.at[pl.ds(st, size), :]
        return wts if k < KM else meta

    def desc(d, k, s, gg, own):
        z_, x_ = s // (2 * X), (s // 2) % X
        return pltpu.make_async_remote_copy(
            src_ref=origin(k) if own else place(k, s, gg),
            dst_ref=place(k, s, gg),
            send_sem=send.at[dirs.index(d), z_ * X + x_, k],
            recv_sem=recv.at[s, k],
            device_id=nbr[d], device_id_type=MESH)

    started = []

    def go(d, k, s, gg, own=False, cond=None):
        conds = [q for q in (has[d], cond) if q is not None]
        cc = None if not conds else functools.reduce(jnp.logical_and, conds)
        when(cc, lambda: desc(d, k, s, gg, own).start())
        started.append((cc, d, k, s, gg, own))

    def take(k, s, gg):
        r = place(k, s, gg)
        pltpu.make_async_copy(r, r, recv.at[s, k]).wait()

    small = [KM, KW]

    def mine(fn):
        for k in range(KW):
            grp = parts[k][2]
            fn(k, g, None if grp < 0 else (g == grp))
        for k in small:
            for q in range(2):
                fn(k + q, q, g == q)

    def theirs(fn, own):
        for k in range(KW):
            grp = parts[k][2]
            if grp >= 0 and not own:
                fn(k, 1 - g, g != grp)
        for k in small:
            for q in range(2):
                fn(k + q, q, g != q)

    def both(a, b):
        if a is None:
            return b
        if b is None:
            return a
        return jnp.logical_and(a, b)

    s0 = at(z, x, c)
    order = {}

    def z0():
        def f(k, gg, cond):
            if k >= KW:
                go("y", k, s0, gg, True, cond)
            go("up", k, s0, gg, True, cond)
            go("dn", k, s0, gg, True, cond)
            go("x", k, s0, gg, True, cond)
            go("c", k, s0, gg, True, cond)
        mine(f)
        for k in range(KW):
            if parts[k][2] >= 0:
                go("c", k, s0, g, True, g != parts[k][2])
        for k in range(KW):
            pltpu.make_async_copy(origin(k), place(k, s0, g), local.at[k]).start()
        pltpu.make_async_copy(wts, place(KW, s0, g), local.at[KW]).start()
        pltpu.make_async_copy(meta, place(KM, s0, g), local.at[KW + 1]).start()

    def zd(d):
        for sg in (-1, 1):
            zz = z + sg * d
            ok = jnp.logical_and(zz >= 0, zz < Z)
            s = at(zz, x, c)

            def f(k, gg, cond):
                cc = both(cond, ok)
                when(cc, lambda: take(k, s, gg))
                if d < Z - 1:
                    go("up" if sg < 0 else "dn", k, s, gg, cond=cc)
                if k >= KW or parts[k][2] >= 0:
                    go("y", k, s, gg, cond=cc)
                go("x", k, s, gg, cond=cc)
                go("c", k, s, gg, cond=cc)
            mine(f)

    def xd(d):
        for sg in ((-1, 1) if d else (1,)):
            zz = z + sg * d
            ok = jnp.logical_and(zz >= 0, zz < Z) if d else None
            s = at(zz, 1 - x, c)

            def f(k, gg, cond):
                cc = both(cond, ok)
                when(cc, lambda: take(k, s, gg))
                if k >= KW or parts[k][2] >= 0:
                    go("y", k, s, gg, cond=cc)
                go("c", k, s, gg, cond=cc)
            mine(f)

    def yd(d, xx):
        for sg in ((-1, 1) if d else (1,)):
            zz = z + sg * d
            ok = jnp.logical_and(zz >= 0, zz < Z) if d else None
            s = at(zz, xx, c)

            def f(k, gg, cond):
                cc = both(cond, ok)
                when(cc, lambda: take(k, s, gg))
                go("c", k, s, gg, cond=cc)
            theirs(f, d == 0 and xx is x)

    z0()
    yd(0, x)
    zd(1)
    xd(0)
    yd(1, x)
    for d in range(2, Z):
        zd(d)
        xd(d - 1)
        yd(d - 2, 1 - x)
        yd(d, x)
    xd(Z - 1)
    yd(Z - 2, 1 - x)
    yd(Z - 1, 1 - x)
    for d in range(Z):
        for xx in (x, 1 - x):
            for sg in ((-1, 1) if d else (1,)):
                zz = z + sg * d
                ok = jnp.logical_and(zz >= 0, zz < Z) if d else None
                s = at(zz, xx, 1 - c)

                def f():
                    for k in range(KW):
                        take(k, s, 0)
                    for q in range(2):
                        take(KW + q, s, q)
                        take(KM + q, s, q)
                when(ok, f)
    for k in range(KW):
        pltpu.make_async_copy(origin(k), place(k, s0, g), local.at[k]).wait()
    pltpu.make_async_copy(wts, place(KW, s0, g), local.at[KW]).wait()
    pltpu.make_async_copy(meta, place(KM, s0, g), local.at[KW + 1]).wait()
    for cc, d, k, s, gg, own in started:
        when(cc, lambda: desc(d, k, s, gg, own).wait_send())


def gather_all(tab, wts, meta, Z, X, parts, cid=0):
    rows, D = tab.shape
    n = 2 * X * Z
    K = len(parts) + 4
    any_ = pl.BlockSpec(memory_space=pl.ANY)
    vm = pl.BlockSpec(memory_space=pltpu.VMEM)
    return pl.pallas_call(
        functools.partial(gather_kernel, Z, X, parts),
        out_shape=[
            jax.ShapeDtypeStruct((n, rows, D), tab.dtype),
            jax.ShapeDtypeStruct((2 * n,) + wts.shape, wts.dtype),
            jax.ShapeDtypeStruct((2 * n,) + meta.shape, meta.dtype),
        ],
        in_specs=[vm, vm, vm],
        out_specs=[any_, any_, any_],
        scratch_shapes=[
            pltpu.SemaphoreType.DMA((5, Z * X, K)),
            pltpu.SemaphoreType.DMA((n, K)),
            pltpu.SemaphoreType.DMA((len(parts) + 2,)),
        ],
        compiler_params=pltpu.CompilerParams(collective_id=cid, has_side_effects=True, vmem_limit_bytes=32 << 20),
        name="gather_all",
    )(tab, wts, meta)


def cut_parts(rows, na, nb, b):
    u = 16
    nbr = int(round(rows * b / u)) * u
    bounds = [0, rows - 2 * nbr, rows - nbr, rows]
    parts = []
    def split(lo, hi, n, grp):
        t = (hi - lo) // u
        cuts = [lo + u * (t * i // n) for i in range(n)] + [hi]
        for i in range(n):
            parts.append((cuts[i], cuts[i + 1] - cuts[i], grp))
    split(bounds[1], bounds[2], nb, 0)
    split(bounds[2], bounds[3], nb, 1)
    split(bounds[0], bounds[1], na, -1)
    return parts


clip_level = 0.002
adam_rate = 0.05
gains_rate = 0.6
rows_rate = 0.05
beta_one = 0.9
beta_two = 0.999
adam_eps = 1e-08
decay_rate = 0.01


def adam_update(weight, first, second, grad, decay, rate):
    first_new = beta_one * first + (1.0 - beta_one) * grad
    second_new = beta_two * second + (1.0 - beta_two) * grad * grad
    fix_one = 1.0 - beta_one**STEP
    fix_two = 1.0 - beta_two**STEP
    weight_new = weight - rate * (
        first_new / fix_one / (jnp.sqrt(second_new / fix_two) + adam_eps) + decay * weight
    )
    return (weight_new, first_new, second_new)


def round_up(n, unit):
    return -(-n // unit) * unit


def digits(ints, base, count):
    return [((ints // base**k) % base).astype(bf16) for k in range(count)]


def small_block(negative_ids, negative_logq, valid_here, width):
    n = negative_ids.shape[0]
    lines = [negative_logq] + digits(negative_ids, 256, 3)
    lines += [jnp.broadcast_to(d, (n,)) for d in digits(valid_here, 256, 2)]
    block = jnp.stack(lines)
    return jnp.pad(block, ((0, 16 - block.shape[0]), (0, width - n)))


def read_small(blocks, n):
    v = blocks[:, :6, :n].astype(f32)
    ids = (v[:, 1] + 256.0 * v[:, 2] + 65536.0 * v[:, 3]).astype(jnp.int32)
    events = jnp.sum(v[:, 4, 0] + 256.0 * v[:, 5, 0])
    return v[:, 0], ids, events


def slot_plan(requests, rows_dev, peers):
    capacity = 2 * requests.shape[0] // peers
    owners = requests // rows_dev
    one_hot = (owners[:, None] == jnp.arange(peers, dtype=jnp.int32)[None, :]).astype(jnp.int32)
    rank_in = jnp.sum((jnp.cumsum(one_hot, 0) - one_hot) * one_hot, 1)
    return owners * capacity + rank_in, capacity


def exchange(blocks):
    return lax.all_to_all(blocks, "row", split_axis=0, concat_axis=0, tiled=True)


def shards(
    shape,
    item_ids,
    lengths,
    target_ids,
    target_logq,
    negative_ids,
    negative_logq,
    table_weight,
    table_accum,
    dense_weight,
    dense_first,
    dense_second,
    gain_weight,
    gain_first,
    gain_second,
):
    groups, peers = shape
    seq_dev, length = item_ids.shape
    rows_dev, width = table_weight.shape
    tokens = seq_dev * length
    n_neg = negative_ids.shape[0]
    X = groups
    Z = peers // (2 * X)
    g = lax.axis_index("grp")
    row_base = lax.axis_index("row") * rows_dev

    table_low = table_weight.astype(bf16)
    dense_low = dense_weight.T.astype(bf16)
    small = small_block(negative_ids, negative_logq, jnp.sum(lengths), width)
    requests = jnp.concatenate([item_ids.reshape(-1), target_ids.reshape(-1), negative_ids])
    slot_at, capacity = slot_plan(requests, rows_dev, peers)
    send_ids = jnp.full((peers * capacity,), -1, jnp.int32).at[slot_at].set(requests)
    asked_ids = exchange(send_ids.reshape(peers, capacity))
    present = asked_ids >= 0

    if (groups, X) == (2, 2):
        rows_pad = round_up(rows_dev, 16)
        padded = jnp.pad(table_low, ((0, rows_pad - rows_dev), (0, 0)))
        table_all, dense_all, small_all = gather_all(
            padded, dense_low, small, Z, X, cut_parts(rows_pad, 2, 2, 0.333)
        )
        neg_bias, neg_ids, event_total = read_small(small_all, n_neg)
        neg_ids = lax.dynamic_slice_in_dim(neg_ids, g * peers, peers, 0).reshape(-1)
        neg_bias = lax.dynamic_slice_in_dim(neg_bias, g * peers, peers, 0).reshape(1, -1)
        wanted = jnp.concatenate([requests[: 2 * tokens], neg_ids])
        wanted = wanted + (rows_pad - rows_dev) * (wanted // rows_dev)
        picked = table_all.reshape(peers * rows_pad, width)[wanted]
        neg_rows = picked[2 * tokens :]
    else:
        dense_all = lax.all_gather(dense_low, ("grp", "row"), axis=0)
        small_all = lax.all_gather(small, ("grp", "row"), axis=0)
        neg_bias, neg_ids, event_total = read_small(small_all, n_neg)
        neg_bias = lax.dynamic_slice_in_dim(neg_bias, g * peers, peers, 0).reshape(1, -1)
        found = table_low[jnp.where(present, asked_ids - row_base, 0)]
        found = jnp.where(present[..., None], found, jnp.zeros_like(found))
        picked = exchange(found).reshape(peers * capacity, width)[slot_at]
        neg_rows = lax.all_gather(picked[2 * tokens :], "row", axis=0, tiled=True)
    hist_rows = picked[:tokens].reshape(seq_dev, length, width)
    target_rows = picked[tokens : 2 * tokens].reshape(seq_dev, length, width)
    dense_all = dense_all.reshape(-1, width)

    inverse = 1.0 / event_total
    d_embedded, d_target, grad_local, neg_local, gain_local, loss_local = seq_step(
        lengths,
        inverse.reshape(1, 1),
        hist_rows,
        target_rows,
        target_logq.astype(f32).reshape(seq_dev, 1, length),
        neg_rows,
        neg_bias,
        dense_all,
        gain_weight,
    )
    gain_local = gain_local[:3]

    dense_grad = lax.psum_scatter(grad_local, ("grp", "row"), scatter_dimension=0, tiled=True).T
    neg_grad = jnp.sum(exchange(neg_local.reshape(peers, n_neg, width)).astype(f32), 0)
    row_grads = jnp.concatenate(
        [d_embedded.reshape(tokens, width), d_target.reshape(tokens, width), neg_grad.astype(bf16)], 0
    ).astype(f32)
    sent = jnp.zeros((peers * capacity, width), f32).at[slot_at].set(row_grads).astype(bf16)
    arrived = exchange(sent.reshape(peers, capacity, width)).astype(f32)
    local_rows = jnp.where(present, asked_ids - row_base, 0).reshape(-1)
    arrived = jnp.where(present[..., None], arrived, 0.0).reshape(-1, width)
    owner_grad = jax.ops.segment_sum(arrived, local_rows, num_segments=rows_dev)
    table_full = lax.psum(owner_grad.astype(bf16), "grp").astype(f32)

    dense_sq = jnp.sum(dense_grad * dense_grad)
    table_sq = jnp.sum(table_full * table_full) / groups
    gain_grad, dense_total, table_total, loss_total = lax.psum(
        (gain_local, dense_sq, table_sq, loss_local[0, 0]), ("grp", "row")
    )
    raw_norm = jnp.sqrt(dense_total + table_total + jnp.sum(gain_grad * gain_grad))
    factor = jnp.minimum(1.0, clip_level / raw_norm)
    table_grad = table_full * factor
    new_accum = table_accum + jnp.mean(table_grad * table_grad, -1)
    new_table = table_weight - rows_rate * table_grad / (jnp.sqrt(new_accum)[:, None] + adam_eps)
    new_dense, new_first, new_second = adam_update(
        dense_weight, dense_first, dense_second, dense_grad * factor, decay_rate, adam_rate
    )
    new_gains, new_gain_first, new_gain_second = adam_update(
        gain_weight, gain_first, gain_second, gain_grad * factor, 0.0, gains_rate
    )
    return (
        loss_total / event_total,
        raw_norm,
        new_table,
        table_grad,
        new_accum,
        new_table.astype(bf16),
        new_dense,
        new_first,
        new_second,
        new_dense.astype(bf16),
        new_gains,
        new_gain_first,
        new_gain_second,
    )


def solution(mesh):
    shape = (mesh.shape["grp"], mesh.shape["row"])
    both = ("grp", "row")
    return jax.shard_map(
        functools.partial(shards, shape),
        mesh=mesh,
        in_specs=(
            P(both, None), P(both), P(both, None), P(both, None), P(both), P(both),
            P("row", None), P("row"), P(None, both), P(None, both), P(None, both),
            P(), P(), P(),
        ),
        out_specs=(
            P(), P(), P("row", None), P("row", None), P("row"), P("row", None),
            P(None, both), P(None, both), P(None, both), P(None, both),
            P(), P(), P(),
        ),
        check_vma=False,
    )
```

```python
import functools

import jax
import jax.numpy as jnp
from jax import lax
from jax.experimental import pallas as pl
from jax.experimental.pallas import tpu as pltpu
from jax.sharding import PartitionSpec as P

HEADS = 8
HDIM = 64
FF = 1024
STEP = 10
f32 = jnp.float32
bf16 = jnp.bfloat16

def mm(a, b):
    return lax.dot_general(a, b, (((1,), (0,)), ((), ())), preferred_element_type=f32)


def mm_t(a, b):
    return lax.dot_general(a, b, (((1,), (1,)), ((), ())), preferred_element_type=f32)


def t_mm(a, b):
    return lax.dot_general(a, b, (((0,), (0,)), ((), ())), preferred_element_type=f32)


GELU_C = 0.7978845608028654


def seq_kernel(
    len_ref, inv_ref,
    hist_ref, tgt_ref, tlq_ref, neg_ref, nlq_ref, wt_ref, gain_ref,
    demb_ref, dtgt_ref, gt_ref, ng_ref, gg_ref,
    emb, xn1, qkv, qh, kh, vh, dch, probs, ctx, aat, xn2, hid, gp, ffn, st, dneg, dst, dhid, dmx, gacc, nacc, rb,
):
    s = pl.program_id(0)
    last = pl.num_programs(0) - 1
    L, D = emb.shape
    inner = HEADS * HDIM
    O1 = 3 * inner
    O2 = O1 + inner
    O3 = O2 + FF
    O4 = O3 + FF
    RB = 128
    NB = L // RB

    @pl.when(s == 0)
    def _():
        @pl.loop(0, D // 16)
        def _(i):
            r = pl.ds(pl.multiple_of(i * 16, 16), 16)
            gacc[r, :] = jnp.zeros((16, gacc.shape[1]), f32)
            nacc[r, :] = jnp.zeros((16, nacc.shape[1]), f32)
        gt_ref[O4:, :] = jnp.zeros((L, D), f32)
        gg_ref[...] = jnp.zeros(gg_ref.shape, f32)

    g1 = gain_ref[0:1, :]
    g2 = gain_ref[1:2, :]
    g3 = gain_ref[2:3, :]

    def rows(i):
        return pl.ds(pl.multiple_of(i * RB, RB), RB)

    def inv_rms(x):
        return lax.rsqrt(jnp.mean(x * x, -1, keepdims=True) + 1e-06)

    @pl.loop(0, NB)
    def _(i):
        r = rows(i)
        x = hist_ref[0, r, :].astype(f32) + wt_ref[pl.ds(pl.multiple_of(O4 + i * RB, RB), RB), :].astype(f32)
        emb[r, :] = x
        xn1[r, :] = (x * inv_rms(x) * g1).astype(bf16)

    qkv[...] = mm_t(xn1[...], wt_ref[0:O1, :]).astype(bf16)

    lane = lax.broadcasted_iota(jnp.int32, (1, 2 * HDIM), 1)

    def own(h):
        return (lane // HDIM) == (h % 2)

    @pl.loop(0, HEADS)
    def _(h):
        m = own(h)
        off = pl.multiple_of((h // 2) * 2 * HDIM, 2 * HDIM)
        zero = jnp.zeros((), bf16)
        qh[h] = jnp.where(m, qkv[:, pl.ds(off, 2 * HDIM)] * jnp.asarray(0.125, bf16), zero)
        kh[h] = jnp.where(m, qkv[:, pl.ds(pl.multiple_of(inner + off, 2 * HDIM), 2 * HDIM)], zero)
        vh[h] = jnp.where(m, qkv[:, pl.ds(pl.multiple_of(2 * inner + off, 2 * HDIM), 2 * HDIM)], zero)

    QB = 256
    NQ = L // QB
    causal = lax.broadcasted_iota(jnp.int32, (QB, QB), 0) >= lax.broadcasted_iota(jnp.int32, (QB, QB), 1)

    @pl.loop(0, HEADS // 2)
    def _(hp):
        off = pl.multiple_of(hp * 2 * HDIM, 2 * HDIM)
        for i in range(NQ):
            n = (i + 1) * QB
            q0 = i * QB
            acc = None
            for j in range(2):
                h = hp * 2 + j
                sc = mm_t(qh[h, q0:q0 + QB, :], kh[h, 0:n, :])
                tail = jnp.where(causal, sc[:, q0:], -1e30)
                sc = tail if i == 0 else jnp.concatenate([sc[:, :q0], tail], 1)
                e = jnp.exp(sc - jnp.max(sc, -1, keepdims=True))
                p = e / jnp.sum(e, -1, keepdims=True)
                probs[h, q0:q0 + QB, 0:n] = p
                c = mm(p.astype(bf16), vh[h, 0:n, :])
                acc = c if acc is None else acc + c
            ctx[q0:q0 + QB, pl.ds(off, 2 * HDIM)] = acc.astype(bf16)

    aat[...] = emb[...] + mm(ctx[...], wt_ref[O1:O2, :])

    @pl.loop(0, NB)
    def _(i):
        r = rows(i)
        x = aat[r, :]
        xn2[r, :] = (x * inv_rms(x) * g2).astype(bf16)

    gp[...] = mm_t(xn2[...], wt_ref[O2:O3, :])

    @pl.loop(0, L // 32)
    def _(i):
        r = pl.ds(pl.multiple_of(i * 32, 32), 32)
        x = gp[r, :]
        x2 = x * x
        t = jnp.tanh(GELU_C * (x + 0.044715 * (x2 * x)))
        half = 0.5 * (1.0 + t)
        hid[r, :] = (x * half).astype(bf16)
        gp[r, :] = half + (0.5 * GELU_C) * x * (1.0 - t * t) * (1.0 + (3 * 0.044715) * x2)

    ffn[...] = aat[...] + mm(hid[...], wt_ref[O3:O4, :])

    @pl.loop(0, NB)
    def _(i):
        r = rows(i)
        x = ffn[r, :]
        st[r, :] = (x * inv_rms(x) * g3).astype(bf16)

    inv = inv_ref[0, 0]
    length = len_ref[s]
    LB = 128
    eye = lax.broadcasted_iota(jnp.int32, (LB, LB), 0) == lax.broadcasted_iota(jnp.int32, (LB, LB), 1)

    @pl.loop(0, L // LB)
    def _(i):
        r = pl.ds(pl.multiple_of(i * LB, LB), LB)
        sl = st[r, :]
        sf = sl.astype(f32)
        tf = tgt_ref[0, r, :].astype(f32)
        tlq = jnp.sum(jnp.where(eye, tlq_ref[0, :, r], 0.0), 1, keepdims=True)
        pos = jnp.sum(sf * tf, -1, keepdims=True) - tlq
        neg = mm_t(sl, neg_ref[...]) - nlq_ref[...]
        top = jnp.maximum(jnp.max(neg, -1, keepdims=True), pos)
        e = jnp.exp(neg - top)
        total = jnp.exp(pos - top) + jnp.sum(e, -1, keepdims=True)
        lt = top + jnp.log(total)
        t_at = i * LB + lax.broadcasted_iota(jnp.int32, (LB, 1), 0)
        valid = (t_at < length).astype(f32)
        gg_ref[3:4, :] += jnp.broadcast_to(jnp.sum(valid * (lt - pos), 0, keepdims=True), (1, D))
        d_pos = valid * inv * (jnp.exp(pos - lt) - 1.0)
        dn = (e * (valid * inv / total)).astype(bf16)
        dneg[r, :] = dn
        dtgt_ref[0, r, :] = (d_pos * sf).astype(bf16)
        dst[r, :] = d_pos * tf + mm(dn, neg_ref[...])

    nacc[...] += t_mm(st[...], dneg[...])

    def norm_back(x, dy, g):
        r = inv_rms(x)
        xh = x * r
        dg = jnp.sum(dy * xh, 0, keepdims=True)
        dyg = dy * g
        dx = r * (dyg - xh * jnp.mean(dyg * xh, -1, keepdims=True))
        return dx, dg

    @pl.loop(0, NB)
    def _(i):
        r = rows(i)
        dx, dg = norm_back(ffn[r, :], dst[r, :], g3)
        gg_ref[2:3, :] += dg
        dst[r, :] = dx
        rb[r, :] = dx.astype(bf16)

    gacc[:, O3:O4] += t_mm(rb[...], hid[...])
    gp[...] = mm_t(rb[...], wt_ref[O3:O4, :]) * gp[...]
    dhid[...] = gp[...].astype(bf16)
    gacc[:, O2:O3] += t_mm(xn2[...], dhid[...])
    ffn[...] = mm(dhid[...], wt_ref[O2:O3, :])

    @pl.loop(0, NB)
    def _(i):
        r = rows(i)
        dx, dg = norm_back(aat[r, :], ffn[r, :], g2)
        gg_ref[1:2, :] += dg
        d = dst[r, :] + dx
        dst[r, :] = d
        rb[r, :] = d.astype(bf16)

    gacc[:, O1:O2] += t_mm(rb[...], ctx[...])
    ctx[...] = mm_t(rb[...], wt_ref[O1:O2, :]).astype(bf16)

    @pl.loop(0, HEADS)
    def _(h):
        off = pl.multiple_of((h // 2) * 2 * HDIM, 2 * HDIM)
        dch[h] = jnp.where(own(h), ctx[:, pl.ds(off, 2 * HDIM)], jnp.zeros((), bf16))

    @pl.loop(0, HEADS // 2)
    def _(hp):
        off = pl.multiple_of(hp * 2 * HDIM, 2 * HDIM)
        dk = [None] * NQ
        dv = [None] * NQ
        for i in range(NQ):
            n = (i + 1) * QB
            q0 = i * QB
            dq = None
            for j in range(2):
                h = hp * 2 + j
                p = probs[h, q0:q0 + QB, 0:n]
                dc = dch[h, q0:q0 + QB, :]
                dp = mm_t(dc, vh[h, 0:n, :])
                ds = (p * (dp - jnp.sum(p * dp, -1, keepdims=True))).astype(bf16)
                pb = p.astype(bf16)
                c = mm(ds, kh[h, 0:n, :])
                dq = c if dq is None else dq + c
                qb = qh[h, q0:q0 + QB, :]
                for b in range(i + 1):
                    k0 = b * QB
                    a = t_mm(ds[:, k0:k0 + QB], qb)
                    dk[b] = a if dk[b] is None else dk[b] + a
                    a = t_mm(pb[:, k0:k0 + QB], dc)
                    dv[b] = a if dv[b] is None else dv[b] + a
            dmx[q0:q0 + QB, pl.ds(off, 2 * HDIM)] = (dq * 0.125).astype(bf16)
        for b in range(NQ):
            k0 = b * QB
            dmx[k0:k0 + QB, pl.ds(pl.multiple_of(inner + off, 2 * HDIM), 2 * HDIM)] = dk[b].astype(bf16)
            dmx[k0:k0 + QB, pl.ds(pl.multiple_of(2 * inner + off, 2 * HDIM), 2 * HDIM)] = dv[b].astype(bf16)

    gacc[:, 0:O1] += t_mm(xn1[...], dmx[...])
    ffn[...] = mm(dmx[...], wt_ref[0:O1, :])

    @pl.loop(0, NB)
    def _(i):
        r = rows(i)
        dx, dg = norm_back(emb[r, :], ffn[r, :], g1)
        gg_ref[0:1, :] += dg
        d = dst[r, :] + dx
        demb_ref[0, r, :] = d.astype(bf16)
        gt_ref[pl.ds(pl.multiple_of(O4 + i * RB, RB), RB), :] += d

    @pl.when(s == last)
    def _():
        @pl.loop(0, O4 // 128)
        def _(i):
            c = pl.ds(pl.multiple_of(i * 128, 128), 128)
            gt_ref[c, :] = gacc[:, c].T

        @pl.loop(0, nacc.shape[1] // 128)
        def _(i):
            c = pl.ds(pl.multiple_of(i * 128, 128), 128)
            ng_ref[c, :] = nacc[:, c].T.astype(bf16)


def seq_step(lengths, inverse, hist, tgt, tlq, neg, nlq, wt, gains, interpret=False):
    S, L, D = hist.shape
    N = neg.shape[0]
    C = wt.shape[0]
    inner = HEADS * HDIM
    whole = lambda *shape: pl.BlockSpec(shape, lambda s: (0,) * len(shape))
    once = lambda *shape: pl.BlockSpec(shape, lambda s: (0,) * len(shape), pipeline_mode=pl.Buffered(1))
    per = pl.BlockSpec((1, L, D), lambda s: (s, 0, 0))
    V = pltpu.VMEM
    return pl.pallas_call(
        seq_kernel,
        grid=(S,),
        in_specs=[
            pl.BlockSpec(memory_space=pltpu.SMEM),
            pl.BlockSpec(memory_space=pltpu.SMEM),
            per, per,
            pl.BlockSpec((1, 1, L), lambda s: (s, 0, 0)),
            once(N, D), once(1, N), once(C, D), once(*gains.shape),
        ],
        out_specs=[per, per, whole(C, D), whole(N, D), whole(8, D)],
        out_shape=[
            jax.ShapeDtypeStruct((S, L, D), bf16),
            jax.ShapeDtypeStruct((S, L, D), bf16),
            jax.ShapeDtypeStruct((C, D), f32),
            jax.ShapeDtypeStruct((N, D), bf16),
            jax.ShapeDtypeStruct((8, D), f32),
        ],
        scratch_shapes=[
            V((L, D), f32), V((L, D), bf16), V((L, 3 * inner), bf16),
            V((HEADS, L, 128), bf16), V((HEADS, L, 128), bf16), V((HEADS, L, 128), bf16), V((HEADS, L, 128), bf16),
            V((HEADS, L, L), f32), V((L, inner), bf16), V((L, D), f32), V((L, D), bf16),
            V((L, FF), bf16), V((L, FF), f32), V((L, D), f32), V((L, D), bf16),
            V((L, N), bf16), V((L, D), f32), V((L, FF), bf16), V((L, 3 * inner), bf16),
            V((D, C - L), f32), V((D, N), f32), V((L, D), bf16),
        ],
        compiler_params=pltpu.CompilerParams(vmem_limit_bytes=60 * 1024 * 1024, dimension_semantics=("arbitrary",)),
        name="seq_step",
        interpret=interpret,
    )(lengths, inverse, hist, tgt, tlq, neg, nlq, wt, gains)


MESH = pl.DeviceIdType.MESH


def gather_kernel(Z, X, parts, tab, wts, meta, table, wfull, mfull, send, recv, local):
    g = lax.axis_index("grp")
    row = lax.axis_index("row")
    z = row // (2 * X)
    x = (row // 2) % X
    c = row % 2
    K = len(parts) + 4
    KW = len(parts)
    KM = KW + 2

    def at(z_, x_, c_):
        return z_ * (2 * X) + x_ * 2 + c_

    nbr = {
        "up": (g, at(z + 1, x, c)), "dn": (g, at(z - 1, x, c)),
        "x": (g, at(z, 1 - x, c)), "y": (1 - g, row), "c": (g, at(z, x, 1 - c)),
    }
    has = {"up": z + 1 < Z, "dn": z > 0, "x": None, "y": None, "c": None}
    dirs = ("up", "dn", "x", "y", "c")

    def when(cond, f):
        if cond is None:
            f()
        else:
            pl.when(cond)(f)

    bar = pltpu.get_barrier_semaphore()
    for d in dirs:
        when(has[d], lambda d=d: pl.semaphore_signal(bar, inc=1, device_id=nbr[d], device_id_type=MESH))
    pl.semaphore_wait(bar, 3 + (z + 1 < Z).astype(jnp.int32) + (z > 0).astype(jnp.int32))

    def place(k, s, gg):
        if k < KW:
            st, size, _ = parts[k]
            return table.at[s, pl.ds(st, size), :]
        if k < KM:
            return wfull.at[gg * (2 * X * Z) + s]
        return mfull.at[gg * (2 * X * Z) + s]

    def origin(k):
        if k < KW:
            st, size, _ = parts[k]
            return tab.at[pl.ds(st, size), :]
        return wts if k < KM else meta

    def desc(d, k, s, gg, own):
        z_, x_ = s // (2 * X), (s // 2) % X
        return pltpu.make_async_remote_copy(
            src_ref=origin(k) if own else place(k, s, gg),
            dst_ref=place(k, s, gg),
            send_sem=send.at[dirs.index(d), z_ * X + x_, k],
            recv_sem=recv.at[s, k],
            device_id=nbr[d], device_id_type=MESH)

    started = []

    def go(d, k, s, gg, own=False, cond=None):
        conds = [q for q in (has[d], cond) if q is not None]
        cc = None if not conds else functools.reduce(jnp.logical_and, conds)
        when(cc, lambda: desc(d, k, s, gg, own).start())
        started.append((cc, d, k, s, gg, own))

    def take(k, s, gg):
        r = place(k, s, gg)
        pltpu.make_async_copy(r, r, recv.at[s, k]).wait()

    small = [KM, KW]

    def mine(fn):
        for k in range(KW):
            grp = parts[k][2]
            fn(k, g, None if grp < 0 else (g == grp))
        for k in small:
            for q in range(2):
                fn(k + q, q, g == q)

    def theirs(fn, own):
        for k in range(KW):
            grp = parts[k][2]
            if grp >= 0 and not own:
                fn(k, 1 - g, g != grp)
        for k in small:
            for q in range(2):
                fn(k + q, q, g != q)

    def both(a, b):
        if a is None:
            return b
        if b is None:
            return a
        return jnp.logical_and(a, b)

    s0 = at(z, x, c)
    order = {}

    def z0():
        def f(k, gg, cond):
            if k >= KW:
                go("y", k, s0, gg, True, cond)
            go("up", k, s0, gg, True, cond)
            go("dn", k, s0, gg, True, cond)
            go("x", k, s0, gg, True, cond)
            go("c", k, s0, gg, True, cond)
        mine(f)
        for k in range(KW):
            if parts[k][2] >= 0:
                go("c", k, s0, g, True, g != parts[k][2])
        for k in range(KW):
            pltpu.make_async_copy(origin(k), place(k, s0, g), local.at[k]).start()
        pltpu.make_async_copy(wts, place(KW, s0, g), local.at[KW]).start()
        pltpu.make_async_copy(meta, place(KM, s0, g), local.at[KW + 1]).start()

    def zd(d):
        for sg in (-1, 1):
            zz = z + sg * d
            ok = jnp.logical_and(zz >= 0, zz < Z)
            s = at(zz, x, c)

            def f(k, gg, cond):
                cc = both(cond, ok)
                when(cc, lambda: take(k, s, gg))
                if d < Z - 1:
                    go("up" if sg < 0 else "dn", k, s, gg, cond=cc)
                if k >= KW or parts[k][2] >= 0:
                    go("y", k, s, gg, cond=cc)
                go("x", k, s, gg, cond=cc)
                go("c", k, s, gg, cond=cc)
            mine(f)

    def xd(d):
        for sg in ((-1, 1) if d else (1,)):
            zz = z + sg * d
            ok = jnp.logical_and(zz >= 0, zz < Z) if d else None
            s = at(zz, 1 - x, c)

            def f(k, gg, cond):
                cc = both(cond, ok)
                when(cc, lambda: take(k, s, gg))
                if k >= KW or parts[k][2] >= 0:
                    go("y", k, s, gg, cond=cc)
                go("c", k, s, gg, cond=cc)
            mine(f)

    def yd(d, xx):
        for sg in ((-1, 1) if d else (1,)):
            zz = z + sg * d
            ok = jnp.logical_and(zz >= 0, zz < Z) if d else None
            s = at(zz, xx, c)

            def f(k, gg, cond):
                cc = both(cond, ok)
                when(cc, lambda: take(k, s, gg))
                go("c", k, s, gg, cond=cc)
            theirs(f, d == 0 and xx is x)

    z0()
    yd(0, x)
    zd(1)
    xd(0)
    yd(1, x)
    for d in range(2, Z):
        zd(d)
        xd(d - 1)
        yd(d - 2, 1 - x)
        yd(d, x)
    xd(Z - 1)
    yd(Z - 2, 1 - x)
    yd(Z - 1, 1 - x)
    for d in range(Z):
        for xx in (x, 1 - x):
            for sg in ((-1, 1) if d else (1,)):
                zz = z + sg * d
                ok = jnp.logical_and(zz >= 0, zz < Z) if d else None
                s = at(zz, xx, 1 - c)

                def f():
                    for k in range(KW):
                        take(k, s, 0)
                    for q in range(2):
                        take(KW + q, s, q)
                        take(KM + q, s, q)
                when(ok, f)
    for k in range(KW):
        pltpu.make_async_copy(origin(k), place(k, s0, g), local.at[k]).wait()
    pltpu.make_async_copy(wts, place(KW, s0, g), local.at[KW]).wait()
    pltpu.make_async_copy(meta, place(KM, s0, g), local.at[KW + 1]).wait()
    for cc, d, k, s, gg, own in started:
        when(cc, lambda: desc(d, k, s, gg, own).wait_send())


def gather_all(tab, wts, meta, Z, X, parts, cid=0):
    rows, D = tab.shape
    n = 2 * X * Z
    K = len(parts) + 4
    any_ = pl.BlockSpec(memory_space=pl.ANY)
    vm = pl.BlockSpec(memory_space=pltpu.VMEM)
    return pl.pallas_call(
        functools.partial(gather_kernel, Z, X, parts),
        out_shape=[
            jax.ShapeDtypeStruct((n, rows, D), tab.dtype),
            jax.ShapeDtypeStruct((2 * n,) + wts.shape, wts.dtype),
            jax.ShapeDtypeStruct((2 * n,) + meta.shape, meta.dtype),
        ],
        in_specs=[vm, vm, vm],
        out_specs=[any_, any_, any_],
        scratch_shapes=[
            pltpu.SemaphoreType.DMA((5, Z * X, K)),
            pltpu.SemaphoreType.DMA((n, K)),
            pltpu.SemaphoreType.DMA((len(parts) + 2,)),
        ],
        compiler_params=pltpu.CompilerParams(collective_id=cid, has_side_effects=True, vmem_limit_bytes=32 << 20),
        name="gather_all",
    )(tab, wts, meta)


def cut_parts(rows, na, nb, b):
    u = 16
    nbr = int(round(rows * b / u)) * u
    bounds = [0, rows - 2 * nbr, rows - nbr, rows]
    parts = []
    def split(lo, hi, n, grp):
        t = (hi - lo) // u
        cuts = [lo + u * (t * i // n) for i in range(n)] + [hi]
        for i in range(n):
            parts.append((cuts[i], cuts[i + 1] - cuts[i], grp))
    split(bounds[1], bounds[2], nb, 0)
    split(bounds[2], bounds[3], nb, 1)
    split(bounds[0], bounds[1], na, -1)
    return parts


MESH = pl.DeviceIdType.MESH


def round_up(n, unit):
    return -(-n // unit) * unit


def plan_kernel(rows_dev, ids_ref, rank_ref, owner_ref, slot_ref):
    peers = slot_ref.shape[0]
    lanes = slot_ref.shape[2]
    P = ids_ref.shape[1]
    KC = 256
    low = lax.broadcasted_iota(jnp.int32, (peers, 1), 0) * rows_dev
    upper = (
        lax.broadcasted_iota(jnp.int32, (KC, KC), 0) < lax.broadcasted_iota(jnp.int32, (KC, KC), 1)
    ).astype(f32).astype(bf16)
    number = lax.broadcasted_iota(jnp.int32, (peers, 1), 0).astype(f32)
    place = lax.broadcasted_iota(jnp.int32, (lanes, 1), 0)
    carry = jnp.zeros((peers, 1), f32)
    lists = jnp.zeros((3 * peers, lanes), f32)
    for k in range(P // KC):
        c = slice(k * KC, (k + 1) * KC)
        ids = ids_ref[:, c]
        own = jnp.logical_and(ids >= low, ids < low + rows_dev).astype(f32)
        ahead = mm(own.astype(bf16), upper) + carry
        rank = jnp.sum(own * ahead, 0, keepdims=True).astype(jnp.int32)
        owner = jnp.sum(own * number, 0, keepdims=True).astype(jnp.int32)
        carry = carry + jnp.sum(own, 1, keepdims=True)
        rank_ref[:, c] = rank
        owner_ref[:, c] = owner
        local = ids - owner * rows_dev
        high = lax.shift_right_logical(local, 6)
        left = local - high * 64
        coded = jnp.concatenate([own, own * left.astype(f32), own * high.astype(f32)], 0)
        lists = lists + mm_t(coded.astype(bf16), (place == rank).astype(f32).astype(bf16))
    there = lists[:peers] > 0.5
    local = lists[peers : 2 * peers] + 64.0 * lists[2 * peers :]
    out = jnp.where(there, local.astype(jnp.int32), -1)
    for j in range(peers):
        slot_ref[j] = out[j : j + 1]


def plan(ids, rows_dev, peers, lanes):
    P = ids.shape[1]
    vm = pl.BlockSpec(memory_space=pltpu.VMEM)
    return pl.pallas_call(
        functools.partial(plan_kernel, rows_dev),
        out_shape=[
            jax.ShapeDtypeStruct((1, P), jnp.int32),
            jax.ShapeDtypeStruct((1, P), jnp.int32),
            jax.ShapeDtypeStruct((peers, 1, lanes), jnp.int32),
        ],
        in_specs=[vm],
        out_specs=[vm, vm, vm],
        compiler_params=pltpu.CompilerParams(vmem_limit_bytes=24 << 20),
        name="plan",
    )(ids)


def xor3(a, b):
    return sum(lax.rem(lax.div(a, m) + lax.div(b, m), 2) * m for m in (1, 2, 4))


def reduce_kernel(
    rows_dev, tail,
    rank_ref, owner_ref, slot_ref, emb_ref, tgt_ref, negid_ref, neg_ref, grad_ref, stat_ref,
    tab_ref, dense_ref, stat_out, tot_out,
    R, stage, rb, idrb, Pacc, nrs, nst, nall, dco, dcr, dstg, drb, dmst, dmr, bst, brv, stc, str_, ssum, tst, trv,
    s_row, r_row, s_id, r_id, s_nrs, r_nrs, s_nag, r_nag, s_dc, r_dc, s_d, r_d, s_dm, r_dm,
    s_b, r_b, s_y, r_y, s_st, r_st, s_t, r_t, loc,
):
    g = lax.axis_index("grp")
    row = lax.axis_index("row")
    h = lax.div(row, 8)
    pos = lax.rem(row, 8)
    c = lax.rem(row, 2)
    q_me = g * 4 + lax.div(pos, 2)
    capr = stage.shape[2]
    main = capr - tail
    T = emb_ref.shape[0]
    rp = tab_ref.shape[0]
    W = 128
    RC = rp
    RZ = rp // 7
    NC = rp // RC
    NB = r_b.shape[0]
    BR = rp // NB

    def remote(src, dst, ss, rs, dev):
        return pltpu.make_async_remote_copy(
            src_ref=src, dst_ref=dst, send_sem=ss, recv_sem=rs, device_id=dev, device_id_type=MESH
        )

    def arrived(ref, sem):
        pltpu.make_async_copy(ref, ref, sem).wait()

    def cube(gg, pp):
        return (gg, h * 8 + pp)

    far = (g, (1 - h) * 8 + pos)

    bar = pltpu.get_barrier_semaphore()
    n_dev = 32
    me = g * 16 + row

    @pl.loop(1, n_dev)
    def _(k):
        o = lax.rem(me + k, n_dev)
        pl.semaphore_signal(bar, inc=1, device_id=(lax.div(o, 16), lax.rem(o, 16)), device_id_type=MESH)
    rank = rank_ref[...]

    @pl.loop(0, capr // 16)
    def _(i):
        r0 = pl.multiple_of(i * 16, 16)
        want = lax.broadcasted_iota(jnp.int32, (16, 1), 0) + r0
        R[pl.ds(r0, 16), :] = (want == rank).astype(f32).astype(bf16)

    KC = 1024

    def build(step):
        ph = lax.div(step, 8)
        t = lax.rem(step, 8)
        zh = h + (1 - ph) * (1 - 2 * h)
        j = zh * 8 + xor3(pos, t)
        acc = None
        for k in range(2 * T // KC):
            cols = slice(k * KC, (k + 1) * KC)
            o = (owner_ref[:, cols] == j).astype(f32).astype(bf16)
            src = emb_ref if k * KC < T else tgt_ref
            r0 = (k * KC) % T
            a = mm(R[:, cols] * o, src[r0:r0 + KC, :])
            acc = a if acc is None else acc + a
        stage[step, 0] = acc[:, :W].astype(bf16)
        stage[step, 1] = acc[:, W:].astype(bf16)

    def row_copies(step, yy):
        ph = lax.div(step, 8)
        t = lax.rem(step, 8)
        zh = h + (1 - ph) * (1 - 2 * h)
        p = xor3(pos, t)
        at = t * 2 + g
        return (
            remote(stage.at[step, yy], rb.at[ph, at], s_row.at[step, yy], r_row.at[ph, at], cube(yy, p)),
            remote(slot_ref.at[zh * 8 + p], idrb.at[ph, at], s_id.at[step, yy], r_id.at[ph, at], cube(yy, p)),
        )

    def self_copies(ph):
        zh = h + (1 - ph) * (1 - 2 * h)
        return (
            pltpu.make_async_copy(stage.at[ph * 8, g], rb.at[ph, g], r_row.at[ph, g]),
            pltpu.make_async_copy(slot_ref.at[zh * 8 + pos], idrb.at[ph, g], r_id.at[ph, g]),
        )

    def send(step):
        for yy in range(2):
            mine = jnp.logical_and(lax.rem(step, 8) == 0, g == yy)

            @pl.when(jnp.logical_not(mine))
            def _():
                for cp in row_copies(step, yy):
                    cp.start()

            @pl.when(mine)
            def _():
                for cp in self_copies(lax.div(step, 8)):
                    cp.start()

    lines = lax.broadcasted_iota(jnp.int32, (RC, 1), 0)

    def add_rows(ph, ids, vals):
        @pl.loop(0, NC)
        def _(i):
            r0 = pl.multiple_of(i * RC, 16)
            hot = (lines == (ids - r0)).astype(f32).astype(bf16)
            Pacc[ph, pl.ds(r0, RC), :] += mm(hot, vals)

    def receive(ph, t):
        for gg in range(2):
            at = t * 2 + gg
            arrived(rb.at[ph, at], r_row.at[ph, at])
            arrived(idrb.at[ph, at], r_id.at[ph, at])
        i0 = idrb[ph, t * 2, :, :main]
        i1 = idrb[ph, t * 2 + 1, :, :main]
        v0 = rb[ph, t * 2, :main, :]
        v1 = rb[ph, t * 2 + 1, :main, :]

        @pl.loop(0, NC)
        def _(i):
            r0 = pl.multiple_of(i * RC, 16)
            a = mm((lines == (i0 - r0)).astype(f32).astype(bf16), v0)
            a = a + mm((lines == (i1 - r0)).astype(f32).astype(bf16), v1)
            Pacc[ph, pl.ds(r0, RC), :] += a

    def tails(ph):
        lane = lax.broadcasted_iota(jnp.int32, (1, W), 1)
        zh = h + (1 - ph) * (1 - 2 * h)
        base = (zh * 8 + pos) * rows_dev
        per = W // tail
        for b in range(16 // per):
            ids = jnp.full((1, W), -1, jnp.int32)
            for k in range(per):
                s = b * per + k
                piece = idrb[ph, s, :, main:main + W]
                if k:
                    piece = pltpu.roll(piece, k * tail, 1)
                ids = jnp.where(lax.div(lane, tail) == k, piece, ids)
            vals = jnp.concatenate([rb[ph, b * per + k, main:, :] for k in range(per)], 0)
            add_rows(ph, ids, vals)
        NG = nall.shape[0]
        for b in range(NG):
            local = negid_ref[:, b * nall.shape[1]:(b + 1) * nall.shape[1]] - base
            add_rows(ph, jnp.where(local < rows_dev, local, -1), nall[b])

    @pl.loop(0, 2 * (rp // RZ))
    def _(i):
        r0 = pl.multiple_of(lax.rem(i, rp // RZ) * RZ, 16)
        Pacc[lax.div(i, rp // RZ), pl.ds(r0, RZ), :] = jnp.zeros((RZ, W), f32)

    build(0)
    pl.semaphore_wait(bar, n_dev - 1)

    core_copy = remote(grad_ref.at[:, 1 - c], dcr, s_dc, r_dc, (g, row + 1 - 2 * c))
    core_copy.start()
    own_copy = pltpu.make_async_copy(grad_ref.at[:, c], dco, loc.at[0])
    own_copy.start()

    nb = nrs.shape[1]

    def nrs_copy(t):
        p = xor3(pos, t)
        return remote(neg_ref.at[pl.ds(pl.multiple_of(p * nb, 16), nb), :], nrs.at[t], s_nrs.at[t], r_nrs.at[t], cube(g, p))

    @pl.loop(1, 8)
    def _(t):
        nrs_copy(t).start()

    def stat_copy(k):
        o = lax.rem(g * 8 + pos + k, 16)
        return remote(stc, str_.at[g * 8 + pos], s_st.at[k], r_st.at[g * 8 + pos], cube(lax.div(o, 8), lax.rem(o, 8)))

    def stat_from(k):
        o = lax.rem(g * 8 + pos + k, 16)
        arrived(str_.at[o], r_st.at[o])

    stat_load = pltpu.make_async_copy(stat_ref, stc, loc.at[1])
    stat_load.start()
    stat_load.wait()
    stat_own = pltpu.make_async_copy(stat_ref, str_.at[g * 8 + pos], loc.at[2])
    stat_own.start()

    @pl.loop(1, 16)
    def _(k):
        stat_copy(k).start()

    def run(lo, hi):
        @pl.loop(lo, hi)
        def _(step):
            build(step)
            send(step - 1)

    run(1, 4)

    @pl.loop(1, 8)
    def _(t):
        arrived(nrs.at[t], r_nrs.at[t])
    total = neg_ref[pl.ds(pl.multiple_of(pos * nb, 16), nb), :].astype(f32)
    for t in range(1, 8):
        total = total + nrs[t].astype(f32)
    nst[0] = total[:, :W].astype(bf16)
    nst[1] = total[:, W:].astype(bf16)

    def nag_copy(t, yy):
        p = xor3(pos, t)
        return remote(
            nst.at[yy], nall.at[g, pl.ds(pl.multiple_of(pos * nb, 16), nb), :],
            s_nag.at[t, yy], r_nag.at[g, pos], cube(yy, p))

    def nag_each(f_remote, f_self):
        @pl.loop(0, 8)
        def _(t):
            for yy in range(2):
                mine = jnp.logical_and(t == 0, g == yy)

                @pl.when(jnp.logical_not(mine))
                def _():
                    f_remote(t, yy)

                if f_self is not None:
                    @pl.when(mine)
                    def _():
                        f_self()

    def nag_self():
        pltpu.make_async_copy(
            nst.at[g], nall.at[g, pl.ds(pl.multiple_of(pos * nb, 16), nb), :], r_nag.at[g, pos]).start()

    run(4, 5)
    nag_each(lambda t, yy: nag_copy(t, yy).start(), nag_self)

    run(5, 16)
    send(jnp.int32(15))

    core_copy.wait_recv()
    own_copy.wait()
    for q in range(8):
        for hh in range(2):
            idx = (q // 4) * 8 + (2 * hh + (q // 2) % 2) * 2 + q % 2
            dstg[q, hh] = (dco[idx] + dcr[idx]).astype(bf16)

    def d_copy(t):
        q = xor3(q_me, t)
        dev = (lax.div(q, 4), h * 8 + lax.rem(q, 4) * 2 + c)
        return remote(dstg.at[q], drb.at[t], s_d.at[t], r_d.at[t], dev)

    @pl.loop(1, 8)
    def _(t):
        d_copy(t).start()

    @pl.loop(0, 8)
    def _(t):
        receive(0, t)

    @pl.loop(0, 16)
    def _(i):
        gg = lax.div(i, 8)
        pp = lax.rem(i, 8)
        ref = nall.at[gg, pl.ds(pl.multiple_of(pp * nb, 16), nb), :]
        arrived(ref, r_nag.at[gg, pp])
    tails(0)

    def b_copy(i):
        ref = pl.ds(pl.multiple_of(i * BR, 16), BR)
        return remote(bst.at[ref, :], brv.at[ref, :], s_b.at[i], r_b.at[i], far)

    @pl.loop(0, NB)
    def _(i):
        ref = pl.ds(pl.multiple_of(i * BR, 16), BR)
        bst[ref, :] = Pacc[0, ref, :].astype(bf16)

        @pl.when(i > 0)
        def _():
            b_copy(i - 1).start()

    b_copy(NB - 1).start()

    stat_own.wait()

    @pl.loop(1, 16)
    def _(k):
        stat_from(k)
    half = str_[0]
    for k in range(1, 16):
        half = half + str_[k]
    ssum[0] = half

    @pl.loop(0, 7)
    def _(t):
        receive(1, t)

    stat_far = remote(ssum.at[0], ssum.at[1], s_st.at[0], r_st.at[16], far)
    stat_far.start()
    receive(1, jnp.int32(7))

    tails(1)

    def y_copy(i):
        ref = tab_ref.at[pl.ds(pl.multiple_of(i * BR, 16), BR), pl.ds(pl.multiple_of(g * W, W), W)]
        return remote(ref, ref, s_y.at[i], r_y.at[i], (1 - g, row))

    d_far = remote(dmst.at[1 - h], dmr, s_dm, r_dm, far)

    def finish(i, sq):
        rr = pl.ds(pl.multiple_of(i * BR, 16), BR)
        arrived(brv.at[rr, :], r_b.at[i])
        low = (Pacc[1, rr, :] + brv[rr, :].astype(f32)).astype(bf16)
        tab_ref[rr, pl.ds(pl.multiple_of(g * W, W), W)] = low

        @pl.when(i > 0)
        def _():
            y_copy(i - 1).start()
        v = low.astype(f32)
        return sq + jnp.sum(v * v, 0, keepdims=True)

    sq = lax.fori_loop(0, NB - 1, finish, jnp.zeros((1, W), f32))

    @pl.loop(1, 8)
    def _(t):
        arrived(drb.at[t], r_d.at[t])
    both = dstg[q_me].astype(f32)
    for t in range(1, 8):
        both = both + drb[t].astype(f32)
    dmst[...] = both.astype(bf16)
    dense_ref[...] = jnp.where(h == 0, both[0], both[1])

    d_far.start()
    sq = finish(NB - 1, sq)
    y_copy(NB - 1).start()
    arrived(dmr, r_dm)
    dense = dense_ref[...] + dmr[...].astype(f32)
    dense_ref[...] = dense
    dsq = jnp.sum(dense * dense, 0, keepdims=True)
    tst[...] = sq + dsq[:, :W] + dsq[:, W:]

    def t_copy(k):
        o = lax.rem(me + k, n_dev)
        return remote(tst, trv.at[me], s_t.at[k], r_t.at[me], (lax.div(o, 16), lax.rem(o, 16)))

    t_own = pltpu.make_async_copy(tst, trv.at[me], loc.at[3])
    t_own.start()

    @pl.loop(1, n_dev)
    def _(k):
        t_copy(k).start()

    arrived(ssum.at[1], r_st.at[16])
    stat_out[...] = ssum[0] + ssum[1]
    t_own.wait()

    @pl.loop(1, n_dev)
    def _(k):
        o = lax.rem(me + k, n_dev)
        arrived(trv.at[o], r_t.at[o])
    tot = trv[0]
    for k in range(1, n_dev):
        tot = tot + trv[k]
    tot_out[...] = tot

    @pl.loop(0, NB)
    def _(i):
        ref = tab_ref.at[pl.ds(pl.multiple_of(i * BR, 16), BR), pl.ds(pl.multiple_of((1 - g) * W, W), W)]
        arrived(ref, r_y.at[i])

    core_copy.wait_send()
    stat_far.wait_send()
    d_far.wait_send()

    @pl.loop(0, NB)
    def _(i):
        b_copy(i).wait_send()
        y_copy(i).wait_send()

    @pl.loop(1, 8)
    def _(t):
        nrs_copy(t).wait_send()
        d_copy(t).wait_send()

    @pl.loop(1, 16)
    def _(k):
        stat_copy(k).wait_send()

    @pl.loop(1, n_dev)
    def _(k):
        t_copy(k).wait_send()

    nag_each(lambda t, yy: nag_copy(t, yy).wait_send(), None)

    @pl.loop(0, 16)
    def _(step):
        for yy in range(2):
            mine = jnp.logical_and(lax.rem(step, 8) == 0, g == yy)

            @pl.when(jnp.logical_not(mine))
            def _():
                for cp in row_copies(step, yy):
                    cp.wait_send()


def reduce_all(rank, owner, slots, emb, tgt, neg_ids, neg, grad, stat, rows_dev, cap, cid=1):
    P = rank.shape[1]
    T, D = emb.shape
    W = 128
    tail = 16
    capr = (cap // 256) * 256 + tail
    rp = round_up(rows_dev, 448)
    lanes = slots.shape[2]
    N = neg.shape[0]
    nd = grad.shape[2]
    NB = 4
    V = pltpu.VMEM
    DMA = pltpu.SemaphoreType.DMA
    vm = pl.BlockSpec(memory_space=pltpu.VMEM)
    any_ = pl.BlockSpec(memory_space=pl.ANY)
    return pl.pallas_call(
        functools.partial(reduce_kernel, rows_dev, tail),
        out_shape=[
            jax.ShapeDtypeStruct((rp, D), bf16),
            jax.ShapeDtypeStruct((nd, D), f32),
            jax.ShapeDtypeStruct((8, D), f32),
            jax.ShapeDtypeStruct((1, W), f32),
        ],
        in_specs=[vm, vm, vm, vm, vm, vm, vm, any_, any_],
        out_specs=[vm, vm, vm, vm],
        scratch_shapes=[
            V((capr, P), bf16), V((16, 2, capr, W), bf16), V((2, 16, capr, W), bf16), V((2, 16, 1, lanes), jnp.int32),
            V((2, rp, W), f32), V((8, N // 8, D), bf16), V((2, N // 8, W), bf16), V((2, N, W), bf16),
            V((16, nd, D), f32), V((16, nd, D), f32), V((8, 2, nd, D), bf16), V((8, 2, nd, D), bf16),
            V((2, nd, D), bf16), V((nd, D), bf16), V((rp, W), bf16), V((rp, W), bf16),
            V((8, D), f32), V((16, 8, D), f32), V((2, 8, D), f32), V((1, W), f32), V((32, 1, W), f32),
            DMA((16, 2)), DMA((2, 16)), DMA((16, 2)), DMA((2, 16)), DMA((8,)), DMA((8,)), DMA((8, 2)), DMA((2, 8)),
            DMA(()), DMA(()), DMA((8,)), DMA((8,)), DMA(()), DMA(()),
            DMA((NB,)), DMA((NB,)), DMA((NB,)), DMA((NB,)), DMA((16,)), DMA((17,)), DMA((32,)), DMA((32,)), DMA((4,)),
        ],
        compiler_params=pltpu.CompilerParams(
            collective_id=cid, has_side_effects=True, vmem_limit_bytes=58 * 1024 * 1024),
        name="reduce_all",
    )(rank, owner, slots, emb, tgt, neg_ids, neg, grad, stat)


clip_level = 0.002
adam_rate = 0.05
gains_rate = 0.6
rows_rate = 0.05
beta_one = 0.9
beta_two = 0.999
adam_eps = 1e-08
decay_rate = 0.01


def adam_update(weight, first, second, grad, decay, rate):
    first_new = beta_one * first + (1.0 - beta_one) * grad
    second_new = beta_two * second + (1.0 - beta_two) * grad * grad
    fix_one = 1.0 - beta_one**STEP
    fix_two = 1.0 - beta_two**STEP
    weight_new = weight - rate * (
        first_new / fix_one / (jnp.sqrt(second_new / fix_two) + adam_eps) + decay * weight
    )
    return (weight_new, first_new, second_new)


def digits(ints, base, count):
    return [((ints // base**k) % base).astype(bf16) for k in range(count)]


def small_block(negative_ids, negative_logq, valid_here, width):
    n = negative_ids.shape[0]
    lines = [negative_logq] + digits(negative_ids, 256, 3)
    lines += [jnp.broadcast_to(d, (n,)) for d in digits(valid_here, 256, 2)]
    block = jnp.stack(lines)
    return jnp.pad(block, ((0, 16 - block.shape[0]), (0, width - n)))


def read_small(blocks, n):
    v = blocks[:, :6, :n].astype(f32)
    ids = (v[:, 1] + 256.0 * v[:, 2] + 65536.0 * v[:, 3]).astype(jnp.int32)
    events = jnp.sum(v[:, 4, 0] + 256.0 * v[:, 5, 0])
    return v[:, 0], ids, events


def slot_plan(requests, rows_dev, peers, capacity):
    owners = requests // rows_dev
    one_hot = (owners[:, None] == jnp.arange(peers, dtype=jnp.int32)[None, :]).astype(jnp.int32)
    rank_in = jnp.sum((jnp.cumsum(one_hot, 0) - one_hot) * one_hot, 1)
    return owners * capacity + rank_in


def exchange(blocks):
    return lax.all_to_all(blocks, "row", split_axis=0, concat_axis=0, tiled=True)


def shards(
    shape,
    item_ids,
    lengths,
    target_ids,
    target_logq,
    negative_ids,
    negative_logq,
    table_weight,
    table_accum,
    dense_weight,
    dense_first,
    dense_second,
    gain_weight,
    gain_first,
    gain_second,
):
    groups, peers = shape
    seq_dev, length = item_ids.shape
    rows_dev, width = table_weight.shape
    tokens = seq_dev * length
    n_neg = negative_ids.shape[0]
    X = groups
    Z = peers // (2 * X)
    g = lax.axis_index("grp")
    row_base = lax.axis_index("row") * rows_dev

    table_low = table_weight.astype(bf16)
    dense_low = dense_weight.T.astype(bf16)
    small = small_block(negative_ids, negative_logq, jnp.sum(lengths), width)
    event_ids = jnp.concatenate([item_ids.reshape(1, -1), target_ids.reshape(1, -1)], 1)
    capacity = 2 * (event_ids.shape[1] + n_neg) // peers
    kernels = (groups, peers) == (2, 16)

    if kernels:
        rows_pad = round_up(rows_dev, 16)
        padded = jnp.pad(table_low, ((0, rows_pad - rows_dev), (0, 0)))
        table_all, dense_all, small_all = gather_all(
            padded, dense_low, small, Z, X, cut_parts(rows_pad, 2, 2, 0.333)
        )
        neg_bias, all_negs, event_total = read_small(small_all, n_neg)
        neg_ids = lax.dynamic_slice_in_dim(all_negs, g * peers, peers, 0).reshape(1, -1)
        neg_bias = lax.dynamic_slice_in_dim(neg_bias, g * peers, peers, 0).reshape(1, -1)
        wanted = jnp.concatenate([event_ids, neg_ids], 1)[0]
        wanted = wanted + (rows_pad - rows_dev) * (wanted // rows_dev)
        picked = table_all.reshape(peers * rows_pad, width)[wanted]
        neg_rows = picked[2 * tokens :]
    else:
        requests = jnp.concatenate([event_ids[0], negative_ids])
        slot_at = slot_plan(requests, rows_dev, peers, capacity)
        send_ids = jnp.full((peers * capacity,), -1, jnp.int32).at[slot_at].set(requests)
        asked_ids = exchange(send_ids.reshape(peers, capacity))
        present = asked_ids >= 0
        dense_all = lax.all_gather(dense_low, ("grp", "row"), axis=0)
        small_all = lax.all_gather(small, ("grp", "row"), axis=0)
        neg_bias, _, event_total = read_small(small_all, n_neg)
        neg_bias = lax.dynamic_slice_in_dim(neg_bias, g * peers, peers, 0).reshape(1, -1)
        found = table_low[jnp.where(present, asked_ids - row_base, 0)]
        found = jnp.where(present[..., None], found, jnp.zeros_like(found))
        picked = exchange(found).reshape(peers * capacity, width)[slot_at]
        neg_rows = lax.all_gather(picked[2 * tokens :], "row", axis=0, tiled=True)
    hist_rows = picked[:tokens].reshape(seq_dev, length, width)
    target_rows = picked[tokens : 2 * tokens].reshape(seq_dev, length, width)
    dense_all = dense_all.reshape(-1, width)

    inverse = 1.0 / event_total
    d_embedded, d_target, grad_local, neg_local, stat_local = seq_step(
        lengths,
        inverse.reshape(1, 1),
        hist_rows,
        target_rows,
        target_logq.astype(f32).reshape(seq_dev, 1, length),
        neg_rows,
        neg_bias,
        dense_all,
        gain_weight,
    )
    d_embedded = d_embedded.reshape(tokens, width)
    d_target = d_target.reshape(tokens, width)

    if kernels:
        rank, owner, lists = plan(event_ids, rows_dev, peers, round_up(capacity, 128))
        table_full, dense_grad, stats, squares = reduce_all(
            rank, owner, lists, d_embedded, d_target, all_negs.reshape(1, -1), neg_local,
            grad_local.reshape(groups * peers // 2, 2, -1, width), stat_local, rows_dev, capacity,
        )
        table_full = table_full[:rows_dev].astype(f32)
        dense_grad = dense_grad.T
        squares = jnp.sum(squares)
    else:
        dense_grad = lax.psum_scatter(grad_local, ("grp", "row"), scatter_dimension=0, tiled=True).T
        neg_grad = jnp.sum(exchange(neg_local.reshape(peers, n_neg, width)).astype(f32), 0)
        row_grads = jnp.concatenate([d_embedded, d_target, neg_grad.astype(bf16)], 0).astype(f32)
        sent = jnp.zeros((peers * capacity, width), f32).at[slot_at].set(row_grads).astype(bf16)
        arrived = exchange(sent.reshape(peers, capacity, width)).astype(f32)
        local_rows = jnp.where(present, asked_ids - row_base, 0).reshape(-1)
        arrived = jnp.where(present[..., None], arrived, 0.0).reshape(-1, width)
        owner_grad = jax.ops.segment_sum(arrived, local_rows, num_segments=rows_dev)
        table_full = lax.psum(owner_grad.astype(bf16), "grp").astype(f32)
        squares = jnp.sum(dense_grad * dense_grad) + jnp.sum(table_full * table_full) / groups
        stats, squares = lax.psum((stat_local, squares), ("grp", "row"))
    gain_grad = stats[:3]
    loss_total = stats[3, 0]
    raw_norm = jnp.sqrt(squares + jnp.sum(gain_grad * gain_grad))
    factor = jnp.minimum(1.0, clip_level / raw_norm)
    table_grad = table_full * factor
    new_accum = table_accum + jnp.mean(table_grad * table_grad, -1)
    new_table = table_weight - rows_rate * table_grad / (jnp.sqrt(new_accum)[:, None] + adam_eps)
    new_dense, new_first, new_second = adam_update(
        dense_weight, dense_first, dense_second, dense_grad * factor, decay_rate, adam_rate
    )
    new_gains, new_gain_first, new_gain_second = adam_update(
        gain_weight, gain_first, gain_second, gain_grad * factor, 0.0, gains_rate
    )
    return (
        loss_total / event_total,
        raw_norm,
        new_table,
        table_grad,
        new_accum,
        new_table.astype(bf16),
        new_dense,
        new_first,
        new_second,
        new_dense.astype(bf16),
        new_gains,
        new_gain_first,
        new_gain_second,
    )


def solution(mesh):
    shape = (mesh.shape["grp"], mesh.shape["row"])
    both = ("grp", "row")
    return jax.shard_map(
        functools.partial(shards, shape),
        mesh=mesh,
        in_specs=(
            P(both, None), P(both), P(both, None), P(both, None), P(both), P(both),
            P("row", None), P("row"), P(None, both), P(None, both), P(None, both),
            P(), P(), P(),
        ),
        out_specs=(
            P(), P(), P("row", None), P("row", None), P("row"), P("row", None),
            P(None, both), P(None, both), P(None, both), P(None, both),
            P(), P(), P(),
        ),
        check_vma=False,
    )
```
